32 devices in a mesh: rep: 4 (over x, core), fsdp: 8 (over z, y).
Axes of the slice: x: 2, y: 2, z: 4, core: 2. Of those that a mesh axis runs over, the one named last changes fastest.
Arguments:
- inputs: bfloat16 [4, 384, 3584], P('rep', 'fsdp'), may hold values from -6 to 6
- cotangent: bfloat16 [4, 384, 3584], P('rep', 'fsdp'), may hold values from -6 to 6
- w_gate: bfloat16 [4, 3584, 14336], P('rep', None, 'fsdp'), may hold values from -6 to 6
- w_up: bfloat16 [4, 3584, 14336], P('rep', None, 'fsdp'), may hold values from -6 to 6
- w_down: bfloat16 [4, 14336, 3584], P('rep', 'fsdp'), may hold values from -6 to 6
- outer_params: float32 [14336, 3584], P('fsdp', 'rep'), may hold values from -6 to 6
- outer_moment: float32 [14336, 3584], P('fsdp', 'rep'), may hold values from -2 to 2
Outputs:
- new_gate: bfloat16 [4, 3584, 14336], P('rep', None, 'fsdp')
- new_up: bfloat16 [4, 3584, 14336], P('rep', None, 'fsdp')
- mixed_down: bfloat16 [4, 14336, 3584], P('rep', 'fsdp')
- new_outer: float32 [14336, 3584], P('fsdp', 'rep')
- new_moment: float32 [14336, 3584], P('fsdp', 'rep')
The draws below stay inside these ranges and needn't reach their ends.
All inputs are finite; a program needn't handle non-finite values.
Results may differ from the reference program's by a relative error of at most 0.0075.
Values may be sent and summed in bfloat16 or wider, within the bound.
A program may use at most 192 MiB of HBM per device.

```python
import math
import jax
import jax.numpy as jnp
from jax import lax

D = 3584
FF = 14336
TOKENS = 384
REPS = 4
N_REP = 4


def level_of(rng, extent, cuts, least, top_value):
    level, own = 1.0, jax.random.fold_in(rng, 6)
    for dim, blocks in cuts:
        steps = jnp.exp(jax.random.uniform(jax.random.fold_in(own, dim), (blocks,), jnp.float32, least / len(cuts), top_value / len(cuts)))
        level = level * jnp.repeat(steps, extent[dim] // blocks).reshape([-1 if axis == dim else 1 for axis in range(len(extent))])
    return level


def scatter_about(stream_key, dims, deviation, limit, cuts=(), dtype=jnp.bfloat16):
    drawn = jax.random.normal(stream_key, dims, jnp.float32) * deviation
    if len(cuts) > 0:
        drawn = level_of(stream_key, dims, cuts, -0.22, 0.18) * drawn
    return jnp.clip(drawn, min=-limit, max=limit).astype(dtype)


def setup_inputs(seed: int = 0) -> dict:
    key_list = jax.random.split(jax.random.key(seed), 8)
    inputs = scatter_about(key_list[0], (REPS, TOKENS, D), 1.0, 6.0, ((0, 4), (1, 8)))
    cotangent = scatter_about(key_list[1], (REPS, TOKENS, D), 1.0, 6.0, ((0, 4), (1, 8)))
    w_gate = scatter_about(key_list[2], (REPS, D, FF), 1.0, 6.0, ((0, 4), (2, 8)))
    w_up = scatter_about(key_list[3], (REPS, D, FF), 1.0, 6.0, ((0, 4), (2, 8)))
    w_down = scatter_about(key_list[4], (REPS, FF, D), 1.0, 6.0, ((0, 4), (1, 8)))
    outer_params = scatter_about(key_list[5], (FF, D), 1.0, 6.0, ((0, 8), (1, 4)), jnp.float32)
    outer_moment = scatter_about(key_list[6], (FF, D), 0.3, 2.0, ((0, 8), (1, 4)), jnp.float32)
    return dict(inputs=inputs, cotangent=cotangent, w_gate=w_gate, w_up=w_up, w_down=w_down, outer_params=outer_params, outer_moment=outer_moment)


step_rate = 2.0
outer_rate = 0.7
moment_keep = 0.9
mix_share = 0.5

def gelu_pair(gate):
    const = math.sqrt(2.0 / math.pi)
    inner = const * (gate + 0.044715 * gate * gate * gate)
    tangent = jnp.tanh(inner)
    active = 0.5 * gate * (1.0 + tangent)
    slope = 0.5 * (1.0 + tangent) + 0.5 * gate * (1.0 - tangent * tangent) * const * (1.0 + 3.0 * 0.044715 * gate * gate)
    return (active, slope)

def inner_step(packed):
    rows, grads_out, wgate, wupper, wdown = packed
    scale_in = D ** (-0.5)
    scale_mid = FF ** (-0.5)
    gate = jnp.dot(rows, wgate, preferred_element_type=jnp.float32) * scale_in
    lifted = jnp.dot(rows, wupper, preferred_element_type=jnp.float32) * scale_in
    active, slope = gelu_pair(gate)
    hidden = (active * lifted).astype(jnp.bfloat16)
    back = jnp.dot(grads_out, wdown.T, preferred_element_type=jnp.float32) * scale_mid
    d_gate = (back * lifted * slope).astype(jnp.bfloat16)
    d_up = (back * active).astype(jnp.bfloat16)
    g_gate = jnp.dot(rows.T, d_gate, preferred_element_type=jnp.float32) * scale_in
    g_up = jnp.dot(rows.T, d_up, preferred_element_type=jnp.float32) * scale_in
    g_down = jnp.dot(hidden.T, grads_out, preferred_element_type=jnp.float32) * scale_mid
    new_gate = (wgate.astype(jnp.float32) - step_rate * g_gate).astype(jnp.bfloat16)
    new_up = (wupper.astype(jnp.float32) - step_rate * g_up).astype(jnp.bfloat16)
    after_down = wdown.astype(jnp.float32) - step_rate * g_down
    return (new_gate, new_up, after_down)

def reference(inputs, cotangent, w_gate, w_up, w_down, outer_params, outer_moment):
    new_gate, new_up, after_down = lax.map(inner_step, (inputs, cotangent, w_gate, w_up, w_down))
    average = lax.optimization_barrier(jnp.sum(w_down.astype(jnp.float32), axis=0)) / N_REP
    delta = outer_params - average
    new_moment = moment_keep * outer_moment + delta
    new_outer = outer_params - outer_rate * (moment_keep * new_moment + delta)
    mixed_down = (mix_share * after_down + (1.0 - mix_share) * new_outer[None]).astype(jnp.bfloat16)
    return (new_gate, new_up, mixed_down, new_outer, new_moment)
```

```python
import functools
import math

import jax
import jax.numpy as jnp
from jax import lax
from jax.experimental import pallas as pl
from jax.experimental.pallas import tpu as pltpu
from jax.sharding import PartitionSpec as P


step_rate = 2.0
outer_rate = 0.7
moment_keep = 0.9
mix_share = 0.5

VMEM_LIMIT = 66 * 1000 * 1000
ANY = pl.BlockSpec(memory_space=pl.ANY)

take_average = outer_rate * (1.0 + moment_keep)
keep_params = 1.0 - take_average
keep_moment = -outer_rate * moment_keep * moment_keep

f32 = jnp.float32
bf16 = jnp.bfloat16


def gelu_pair(gate):
    const = math.sqrt(2.0 / math.pi)
    square = gate * gate
    tangent = jnp.tanh(const * (gate + 0.044715 * square * gate))
    half = 0.5 * (1.0 + tangent)
    active = gate * half
    slope = half + 0.5 * gate * (1.0 - tangent * tangent) * const * (1.0 + 3.0 * 0.044715 * square)
    return (active, slope)


def divide(extent, most, unit):
    for parts in range(most, 0, -1):
        if extent % (parts * unit) == 0:
            return parts
    return 1


def params(**more):
    return pltpu.CompilerParams(vmem_limit_bytes=VMEM_LIMIT, **more)


def cost(flops, moved):
    return pl.CostEstimate(flops=int(flops), bytes_accessed=int(moved), transcendentals=0)


def forward_body(scale_in, scale_mid, x_ref, c_ref, wg_ref, wu_ref, wd_ref, h_ref, dg_ref, du_ref):
    gate = jnp.dot(x_ref[...], wg_ref[...], preferred_element_type=f32) * scale_in
    lifted = jnp.dot(x_ref[...], wu_ref[...], preferred_element_type=f32) * scale_in
    back = (
        lax.dot_general(
            c_ref[...], wd_ref[...], (((1,), (1,)), ((), ())), preferred_element_type=f32
        )
        * scale_mid
    )
    active, slope = gelu_pair(gate)
    h_ref[...] = (active * lifted).T.astype(bf16)
    dg_ref[...] = (back * lifted * slope).astype(bf16)
    du_ref[...] = (back * active).astype(bf16)


def forward(rows, cots, wg, wu, wd, scale_in, scale_mid):
    tokens, d = rows.shape
    ff = wg.shape[1]
    tf = ff // divide(ff, 8, 128)
    tt = tokens // divide(tokens, max(1, tokens // 384), 128)
    grid = (ff // tf, tokens // tt)
    tok = pl.BlockSpec((tt, d), lambda i, j: (j, 0))
    col = pl.BlockSpec((d, tf), lambda i, j: (0, i))
    out = pl.BlockSpec((tt, tf), lambda i, j: (j, i))
    return pl.pallas_call(
        functools.partial(forward_body, scale_in, scale_mid),
        grid=grid,
        in_specs=[tok, tok, col, col, pl.BlockSpec((tf, d), lambda i, j: (i, 0))],
        out_specs=[pl.BlockSpec((tf, tt), lambda i, j: (i, j)), out, out],
        out_shape=[
            jax.ShapeDtypeStruct((ff, tokens), bf16),
            jax.ShapeDtypeStruct((tokens, ff), bf16),
            jax.ShapeDtypeStruct((tokens, ff), bf16),
        ],
        compiler_params=params(),
        cost_estimate=cost(6 * tokens * d * ff, 6 * d * ff + 10 * tokens * d),
        name="forward",
    )(rows, cots, wg, wu, wd)


def update_body(scale, x_ref, dg_ref, du_ref, wg_ref, wu_ref, ng_ref, nu_ref):
    for d_ref, w_ref, o_ref in ((dg_ref, wg_ref, ng_ref), (du_ref, wu_ref, nu_ref)):
        grad = jnp.dot(x_ref[...], d_ref[...], preferred_element_type=f32)
        o_ref[...] = (w_ref[...].astype(f32) - scale * grad).astype(bf16)


def update(turned, d_gate, d_up, wg, wu, scale):
    d, tokens = turned.shape
    ff = wg.shape[1]
    td = d // divide(d, 7, 128)
    weight = pl.BlockSpec((td, ff), lambda i: (i, 0))
    grads = pl.BlockSpec((tokens, ff), lambda i: (0, 0))
    return pl.pallas_call(
        functools.partial(update_body, scale),
        grid=(d // td,),
        in_specs=[pl.BlockSpec((td, tokens), lambda i: (i, 0)), grads, grads, weight, weight],
        out_specs=[weight, weight],
        out_shape=[jax.ShapeDtypeStruct(wg.shape, bf16)] * 2,
        compiler_params=params(),
        cost_estimate=cost(4 * tokens * d * ff, 8 * d * ff),
        name="update",
    )(turned, d_gate, d_up, wg, wu)


def join_body(*refs):
    blocks, (x_ref, c_ref, t_ref) = refs[:-3], refs[-3:]
    half = blocks[0].shape[0] // 2
    for i, block in enumerate(blocks):
        x_ref[i * half : (i + 1) * half, :] = block[:half, :]
        c_ref[i * half : (i + 1) * half, :] = block[half:, :]
    t_ref[...] = x_ref[...].T


def join(blocks):
    pair, d = blocks[0].shape
    tokens = len(blocks) * pair // 2
    td = d // divide(d, 7, 128)
    out = pl.BlockSpec((tokens, td), lambda i: (0, i))
    return pl.pallas_call(
        join_body,
        grid=(d // td,),
        in_specs=[pl.BlockSpec((pair, td), lambda i: (0, i))] * len(blocks),
        out_specs=[out, out, pl.BlockSpec((td, tokens), lambda i: (i, 0))],
        out_shape=[
            jax.ShapeDtypeStruct((tokens, d), bf16),
            jax.ShapeDtypeStruct((tokens, d), bf16),
            jax.ShapeDtypeStruct((d, tokens), bf16),
        ],
        compiler_params=params(),
        cost_estimate=cost(2e6, 10 * tokens * d),
        name="join",
    )(*blocks)


def pack_body(r_ref, w_ref, o_ref):
    o_ref[...] = w_ref[...]


def pack(rep, wd, chunk, unit, width):
    start, units = chunk
    return pl.pallas_call(
        pack_body,
        grid_spec=pltpu.PrefetchScalarGridSpec(
            num_scalar_prefetch=1,
            grid=(units, 2),
            in_specs=[
                pl.BlockSpec((unit, width), lambda j, i, r: (start + j, (r[0] ^ 1) ^ (2 * i)))
            ],
            out_specs=pl.BlockSpec((unit, width), lambda j, i, r: (j, i)),
        ),
        out_shape=jax.ShapeDtypeStruct((units * unit, 2 * width), bf16),
        compiler_params=params(),
        cost_estimate=cost(2e6, 8 * units * unit * width),
        name="pack",
    )(rep, wd)


def sums_body(count, r_ref, own_ref, far_ref, near_ref, p_ref, m_ref, o_ref):
    width = own_ref.shape[1]
    far = far_ref[...].astype(f32) + near_ref[:, width:].astype(f32)
    own = own_ref[...].astype(f32) + near_ref[:, :width].astype(f32)
    o_ref[:, :width] = far.astype(bf16)
    o_ref[:, width:] = (
        keep_params * p_ref[...] + keep_moment * m_ref[...] + (take_average / count) * own
    ).astype(bf16)


def row_specs(chunk, unit, width):
    start, _ = chunk
    own = pl.BlockSpec((unit, width), lambda i, r: (start + i, r[0]))
    far = pl.BlockSpec((unit, width), lambda i, r: (start + i, r[0] ^ 2))
    pair = pl.BlockSpec((unit, 2 * width), lambda i, r: (i, 0))
    state = pl.BlockSpec((unit, width), lambda i, r: (start + i, 0))
    return own, far, pair, state


def sums(rep, wd, near, op, om, chunk, unit, width, count):
    units = chunk[1]
    own, far, pair, state = row_specs(chunk, unit, width)
    return pl.pallas_call(
        functools.partial(sums_body, count),
        grid_spec=pltpu.PrefetchScalarGridSpec(
            num_scalar_prefetch=1,
            grid=(units,),
            in_specs=[own, far, pair, state, state],
            out_specs=pair,
        ),
        out_shape=jax.ShapeDtypeStruct((units * unit, 2 * width), bf16),
        compiler_params=params(),
        cost_estimate=cost(2e6, 20 * units * unit * width),
        name="sums",
    )(rep, wd, wd, near, op, om)


def outer_body(count, r_ref, own_ref, far_ref, near_ref, cross_ref, p_ref, m_ref, *rest):
    no_ref, nm_ref, pair_ref = rest[-3:]
    width = own_ref.shape[1]
    own = own_ref[...].astype(f32) + near_ref[:, :width].astype(f32)
    far = far_ref[...].astype(f32) + near_ref[:, width:].astype(f32)
    params_now = p_ref[...]
    delta = params_now - (own + cross_ref[:, :width].astype(f32)) / count
    moment = moment_keep * m_ref[...] + delta
    fresh = params_now - outer_rate * (moment_keep * moment + delta)
    nm_ref[...] = moment
    no_ref[...] = fresh
    pair_ref[:, :width] = fresh.astype(bf16)
    pair_ref[:, width:] = (
        cross_ref[:, width:].astype(f32) + (take_average / count) * far
    ).astype(bf16)


def outer(rep, wd, near, cross, op, om, before, after, chunk, unit, width, count):
    units = chunk[1]
    own, far, pair, state = row_specs(chunk, unit, width)
    return pl.pallas_call(
        functools.partial(outer_body, count),
        grid_spec=pltpu.PrefetchScalarGridSpec(
            num_scalar_prefetch=1,
            grid=(units,),
            in_specs=[own, far, pair, pair, state, state] + [ANY] * len(before + after),
            out_specs=[state, state, pair],
        ),
        out_shape=[
            jax.ShapeDtypeStruct(op.shape, f32),
            jax.ShapeDtypeStruct(op.shape, f32),
            jax.ShapeDtypeStruct((units * unit, 2 * width), bf16),
        ],
        input_output_aliases={7: 0, 8: 1} if before else {},
        compiler_params=params(),
        cost_estimate=cost(2e6, 28 * units * unit * width),
        name="outer",
    )(rep, wd, wd, near, cross, op, om, *before, *after)


def mixed_body(scale, r_ref, h_ref, c_ref, w_ref, mine_ref, theirs_ref, *rest):
    o_ref = rest[-1]
    grad = jnp.dot(h_ref[...], c_ref[...], preferred_element_type=f32)
    fresh = jnp.where(pl.program_id(0) < 2, mine_ref[...], theirs_ref[...]).astype(f32)
    after = w_ref[...].astype(f32) - scale * grad
    o_ref[...] = (mix_share * after + (1.0 - mix_share) * fresh).astype(bf16)


def mixed(rep, hidden, cots, wd, mine, theirs, before, chunk, unit, width, scale):
    start, units = chunk
    tokens = hidden.shape[1]

    def column(i, r):
        return r[0] ^ (2 * (i % 2) + i // 2)

    weight = pl.BlockSpec((unit, width), lambda i, j, r: (start + j, column(i, r)))
    return pl.pallas_call(
        functools.partial(mixed_body, scale),
        grid_spec=pltpu.PrefetchScalarGridSpec(
            num_scalar_prefetch=1,
            grid=(4, units),
            in_specs=[
                pl.BlockSpec((unit, tokens), lambda i, j, r: (start + j, 0)),
                pl.BlockSpec((tokens, width), lambda i, j, r: (0, column(i, r))),
                weight,
                pl.BlockSpec(
                    (unit, width),
                    lambda i, j, r: (jnp.where(i < 2, j, units - 1), jnp.minimum(i, 1)),
                ),
                pl.BlockSpec(
                    (unit, width),
                    lambda i, j, r: (jnp.where(i < 2, 0, j), jnp.maximum(i - 2, 0)),
                ),
            ]
            + [ANY] * len(before),
            out_specs=weight,
        ),
        out_shape=jax.ShapeDtypeStruct(wd.shape, bf16),
        input_output_aliases={6: 0} if before else {},
        compiler_params=params(),
        cost_estimate=cost(8 * tokens * units * unit * width, 24 * units * unit * width),
        name="mixed",
    )(rep, hidden, cots, wd, mine, theirs, *before)


def per_device(inputs, cotangent, w_gate, w_up, w_down, outer_params, outer_moment):
    d = w_gate.shape[1]
    shards = lax.axis_size("fsdp")
    ff = w_gate.shape[2] * shards
    scale_in = d ** (-0.5)
    scale_mid = ff ** (-0.5)
    wg, wu, wd = w_gate[0], w_up[0], w_down[0]
    count = lax.axis_size("rep")
    rep = lax.axis_index("rep").astype(jnp.int32).reshape(1)
    width = outer_params.shape[1]
    parts = divide(wd.shape[0], 8, 16)
    unit = wd.shape[0] // parts
    inner = parts - 2
    lengths = [n for n in (1, inner - inner // 2, inner // 2, 1) if n > 0]
    chunks = [(sum(lengths[:i]), n) for i, n in enumerate(lengths)]

    order = list(range(0, shards, 2)) + list(range(1, shards, 2))[::-1]
    forth = [(order[i], order[(i + 1) % shards]) for i in range(shards)]
    back = [(b, a) for a, b in forth]
    flip_core = [(i, i ^ 1) for i in range(count)]
    flip_chip = [(i, i ^ 2) for i in range(count)]

    longer, shorter = shards // 2, shards - 1 - shards // 2
    near, cross, packed, ready = [], [], [], []
    own = jnp.concatenate([inputs[0], cotangent[0]], axis=0)
    one, two = [own], [own]

    def hop(step):
        if step < longer:
            one.append(lax.ppermute(one[-1], "fsdp", forth))
        if step < shorter:
            two.append(lax.ppermute(two[-1], "fsdp", back))

    hop(0)
    for chunk in chunks:
        packed.append(pack(rep, wd, chunk, unit, width))
        near.append(lax.ppermute(packed[-1], "rep", flip_core))
    for chunk, other in zip(chunks, near):
        ready.append(sums(rep, wd, other, outer_params, outer_moment, chunk, unit, width, count))
        cross.append(lax.ppermute(ready[-1], "rep", flip_chip))
    for step in range(1, longer):
        hop(step)
    rows, cots, turned = join(one + two[:0:-1])

    hidden, d_gate, d_up = forward(rows, cots, wg, wu, wd, scale_in, scale_mid)
    new_gate, new_up = update(turned, d_gate, d_up, wg, wu, step_rate * scale_in)

    state, out = (), ()
    for k, chunk in enumerate(chunks):
        after = (hidden,) if k < 2 else (new_gate,)
        new_outer, new_moment, mine = outer(
            rep, wd, near[k], cross[k], outer_params, outer_moment, state, after, chunk,
            unit, width, count,
        )
        state = (new_outer, new_moment)
        theirs = lax.ppermute(mine, "rep", flip_core)
        out = (
            mixed(
                rep, hidden, cots, wd, mine, theirs, out, chunk, unit, width,
                step_rate * scale_mid,
            ),
        )
    return (new_gate[None], new_up[None], out[0][None], new_outer, new_moment)


def solution(mesh):
    in_specs = (
        P("rep", "fsdp", None),
        P("rep", "fsdp", None),
        P("rep", None, "fsdp"),
        P("rep", None, "fsdp"),
        P("rep", "fsdp", None),
        P("fsdp", "rep"),
        P("fsdp", "rep"),
    )
    out_specs = (
        P("rep", None, "fsdp"),
        P("rep", None, "fsdp"),
        P("rep", "fsdp", None),
        P("fsdp", "rep"),
        P("fsdp", "rep"),
    )
    return jax.shard_map(
        per_device, mesh=mesh, in_specs=in_specs, out_specs=out_specs, check_vma=False
    )
```
